32 devices in a mesh: spin: 2 (over x), row: 4 (over z), col: 4 (over y, core).
Axes of the slice: x: 2, y: 2, z: 4, core: 2. Of those that a mesh axis runs over, the one named last changes fastest.
Arguments:
- hamiltonian: float32 [7168, 3584], P(('spin', 'row'), 'col'), parts along dimension 0
- bounds: float32 [4], P('spin'), parts along dimension 0
- n_occ: int32 [2], P('spin'), parts along dimension 0
Outputs:
- output 1: float32 [7168, 3584], P(('spin', 'row'), 'col'), parts along dimension 0
- output 2: float32 [2], P('spin'), parts along dimension 0
There are 2 independent parts. The reference program is written for one: setup_inputs(seed, part) draws one part's arguments, and reference() takes and returns one part's arrays. A program takes and returns all parts, laid end to end along the dimension named above; each array names one.
All inputs are finite; a program needn't handle non-finite values.
Results may differ from the reference program's by a relative error of at most 0.001.
Values sent between devices are 32-bit elements.
A program may use at most 1 GiB of HBM per device.

```python
import jax
import jax.numpy as jnp
from jax import lax

N = 3584
STEPS = 3


def setup_inputs(seed: int = 0, part: int = 0) -> dict:
    key = jax.random.fold_in(jax.random.key(seed), part)
    k_off, k_diag, k_shift, k_margin, k_occ = jax.random.split(key, 5)
    gauss_mat = jax.random.normal(k_off, (N, N), jnp.float32)
    sym_part = (gauss_mat + gauss_mat.T) * (2.0 * N) ** -0.5
    unif_diag = jax.random.uniform(k_diag, (N,), jnp.float32)
    shift_val = 2.0 + jax.random.uniform(k_shift, (), jnp.float32)
    diag_vals = shift_val + 0.8 * (3.0 * unif_diag * unif_diag - 1.0)
    index_vec = jnp.arange(N)
    on_diag = index_vec[:, None] == index_vec[None, :]
    hamiltonian = jnp.where(on_diag, diag_vals[None, :], sym_part)
    margins = jax.random.uniform(k_margin, (2,), jnp.float32, 0.0, 0.5)
    bounds = jnp.stack([jnp.min(diag_vals) - 2.4 - margins[0], jnp.max(diag_vals) + 2.4 + margins[1]])
    n_occ = jax.random.randint(k_occ, (1,), 3 * N // 20, 7 * N // 20 + 1, jnp.int32)
    return {"hamiltonian": hamiltonian, "bounds": bounds, "n_occ": n_occ}


def reference(hamiltonian, bounds, n_occ):
    occupied = n_occ[0].astype(jnp.float32)
    mu_val = jnp.trace(hamiltonian) / N
    lam_scale = jnp.minimum(occupied / (bounds[1] - mu_val), (N - occupied) / (mu_val - bounds[0]))
    identity = jnp.eye(N, dtype=jnp.float32)
    density = (lam_scale / N) * (mu_val * identity - hamiltonian) + (occupied / N) * identity

    def purify_step(dens_cur, unused_x):
        dens_sq = jnp.dot(dens_cur, dens_cur, preferred_element_type=jnp.float32, precision=lax.Precision.HIGHEST)
        dens_cube = jnp.dot(dens_sq, dens_cur, preferred_element_type=jnp.float32, precision=lax.Precision.HIGHEST)
        trace_x = jnp.trace(dens_cur)
        trace_sq = jnp.sum(dens_cur * dens_cur)
        trace_cube = jnp.sum(dens_sq * dens_cur)
        mix_coef = (trace_sq - trace_cube) / (trace_x - trace_sq)
        updated = ((1.0 - 2.0 * mix_coef) * dens_cur + (1.0 + mix_coef) * dens_sq - dens_cube) / (1.0 - mix_coef)
        return updated, None

    density, _ = lax.scan(purify_step, density, None, length=STEPS)
    energy = 2.0 * jnp.sum(density * hamiltonian)
    return density, energy[None]
```

```python
import functools

import jax
import jax.numpy as jnp
from jax import lax
from jax.experimental import pallas as pl
from jax.experimental.pallas import tpu as pltpu
from jax.sharding import PartitionSpec as P

STEPS = 3
GRID = 4
HIGHEST = lax.Precision.HIGHEST
MESH = pl.DeviceIdType.MESH
VMEM_BYTES = 62 * 2**20
BLOCKS = ((0, 0), (0, 1), (0, 2), (1, 1), (1, 2), (2, 2), (2, 3), (3, 3), (3, 0), (3, 1))
NB = len(BLOCKS)
EARLY = (3, 5)
ORDER = (
    (0, 1, 2, 3, 4, 5, 6, 7, 8, 9),
    (3, 4, 0, 5, 1, 6, 2, 7, 8, 9),
    (5, 6, 7, 3, 8, 4, 9, 0, 1, 2),
    (7, 8, 9, 5, 6, 3, 4, 0, 1, 2),
)
LAG = 2


def pick(index, values):
    out = jnp.int32(values[-1])
    for k in range(len(values) - 2, -1, -1):
        out = jnp.where(index == k, jnp.int32(values[k]), out)
    return out


def order_of(z, t):
    return pick(z, [0] * GRID) + sum(jnp.where(z == k, pick(t, ORDER[k]), 0) for k in range(GRID))


def block_of(i, j):
    table = [0] * (GRID * GRID)
    for b, (bi, bj) in enumerate(BLOCKS):
        table[bi * GRID + bj] = b
        table[bj * GRID + bi] = b
    stored = [1 if (k // GRID, k % GRID) in BLOCKS else 0 for k in range(GRID * GRID)]
    at = i * GRID + j
    return pick(at, table), pick(at, stored)


def remote(src, dst, send_sem, recv_sem, z, q):
    return pltpu.make_async_remote_copy(
        src_ref=src, dst_ref=dst, send_sem=send_sem, recv_sem=recv_sem, device_id={"row": z, "col": q}, device_id_type=MESH
    )


def group_barrier(z, q):
    barrier = pltpu.get_barrier_semaphore()
    me = z * GRID + q

    def signal(k, carry):
        to = (me + k) % (GRID * GRID)
        pl.semaphore_signal(barrier, inc=1, device_id={"row": to // GRID, "col": to % GRID}, device_id_type=MESH)
        return carry

    lax.fori_loop(1, GRID * GRID, signal, 0)
    pl.semaphore_wait(barrier, GRID * GRID - 1)


def reduce_copy(k, me, red, send_sems, recv_sems):
    to = (me + k) % (GRID * GRID)
    return remote(red.at[me], red.at[me], send_sems.at[k], recv_sems.at[me], to // GRID, to % GRID)


def reduce_start(me, red, send_sems, recv_sems):
    def body(k, carry):
        reduce_copy(k, me, red, send_sems, recv_sems).start()
        return carry

    lax.fori_loop(1, GRID * GRID, body, 0)


def reduce_finish(me, red, send_sems, recv_sems):
    def body(k, carry):
        frm = (me + k) % (GRID * GRID)
        remote(red.at[frm], red.at[frm], send_sems.at[k], recv_sems.at[frm], frm // GRID, frm % GRID).wait_recv()
        reduce_copy(k, me, red, send_sems, recv_sems).wait_send()
        return carry

    lax.fori_loop(1, GRID * GRID, body, 0)
    return jnp.sum(red[...], axis=0)


def as_tile(*sums):
    row = lax.broadcasted_iota(jnp.int32, (8, 128), 0)
    tile = jnp.zeros((8, 128), jnp.float32)
    for k, value in enumerate(sums):
        tile = jnp.where(row == k, value, tile)
    return tile


def prepare_kernel(order, ham, bounds, n_occ, ham_strip, dens, red, send_sem, recv_sem, red_send, red_recv):
    z, q = lax.axis_index("row"), lax.axis_index("col")
    me = z * GRID + q
    rows, cols = ham.shape[1:]
    local_row = lax.broadcasted_iota(jnp.int32, (rows, cols), 0)
    local_col = lax.broadcasted_iota(jnp.int32, (rows, cols), 1)
    group_barrier(z, q)

    def exchange(k):
        to = (q + k) % GRID
        return remote(ham.at[to], ham_strip.at[q], send_sem.at[k], recv_sem.at[q], z, to)

    for k in (2, 3, 1):
        exchange(k).start()
    part = jnp.float32(0.0)
    for s in range(GRID):
        part += jnp.sum(jnp.where((local_row + s * rows == local_col) & (z == q), ham[s], 0.0))
    red[me] = as_tile(part)
    ham_strip[q] = ham[q]
    reduce_start(me, red, red_send, red_recv)
    total = reduce_finish(me, red, red_send, red_recv)
    mu = total[0:1, 0:1] / order
    occ = n_occ[0].astype(jnp.float32)
    occ_v = jnp.full((1, 1), occ)
    low, high = jnp.full((1, 1), bounds[0]), jnp.full((1, 1), bounds[1])
    lam = jnp.minimum(occ_v / (high - mu), (order - occ_v) / (mu - low))
    scale, shift = lam / order, occ_v / order

    def write(j):
        on_diag = (local_row + q * rows == local_col) & (z == j)
        dens[j] = scale * (jnp.where(on_diag, mu, 0.0) - ham_strip[j]) + jnp.where(on_diag, shift, 0.0)

    write(q)
    for k in (1, 2, 3):
        frm = (q + k) % GRID
        remote(ham.at[0], ham_strip.at[frm], send_sem.at[k], recv_sem.at[frm], z, frm).wait_recv()
        write(frm)
    for k in (1, 2, 3):
        exchange(k).wait_send()


def step_kernel(last, *refs):
    if last:
        strip, ham_strip, out, energy, xall, sq, res, red, red2 = refs[:9]
        recv, sent, red_send, red_recv, red2_send, red2_recv, out_send, out_recv = refs[9:]
    else:
        strip, out, xall, sq, red = refs[:5]
        recv, sent, red_send, red_recv = refs[5:]
        res = out
    z, q = lax.axis_index("row"), lax.axis_index("col")
    me = z * GRID + q
    other = (q + 2) % GRID
    mate = q + 1 - 2 * (q % 2)
    mate_other = (mate + 2) % GRID
    rows, cols = strip.shape[1:]
    local_row = lax.broadcasted_iota(jnp.int32, (rows, cols), 0)
    local_col = lax.broadcasted_iota(jnp.int32, (rows, cols), 1)
    row_of = [i for i, _ in BLOCKS]
    col_of = [j for _, j in BLOCKS]

    def is_early(b):
        return functools.reduce(jnp.logical_or, [b == e for e in EARLY])

    def hop(src, b, s, line, kind, z_to, q_to):
        return remote(src, xall.at[b, s], sent.at[b, line, kind], recv.at[b, s], z_to, q_to)

    def forward(src, b, s, line, cross, act):
        origin = pick(b, row_of)

        @pl.when((z >= origin) & (z < GRID - 1) & cross[0])
        def _():
            act(hop(src, b, s, line, 0, z + 1, q))

        @pl.when((z <= origin) & (z > 0) & cross[0])
        def _():
            act(hop(src, b, s, line, 1, z - 1, q))

        if line == 0:

            @pl.when(cross[1])
            def _():
                act(hop(src, b, s, line, 2, z, other))

        act(hop(src, b, s, line, 3, z, mate))

    def arrived(b, s):
        remote(xall.at[b, s], xall.at[b, s], sent.at[b, 0, 0], recv.at[b, s], z, mate).wait_recv()

    def start(copy):
        copy.start()

    def wait_send(copy):
        copy.wait_send()

    def own_lines(t, act, waits):
        b = order_of(z, t)
        origin, col = pick(b, row_of), pick(b, col_of)
        early = is_early(b)

        @pl.when(origin == z)
        def _():
            forward(strip.at[col], b, q, 0, (True, True), act)

        @pl.when(origin != z)
        def _():
            if waits:
                arrived(b, q)
            forward(xall.at[b, q], b, q, 0, (True, jnp.logical_not(early)), act)

        @pl.when(early)
        def _():
            if waits:
                arrived(b, other)
            forward(xall.at[b, other], b, other, 1, (True, False), act)

    def late_line(b, act, waits):
        @pl.when(jnp.logical_not(is_early(b)))
        def _():
            if waits:
                arrived(b, other)
            act(hop(xall.at[b, other], b, other, 1, 3, z, mate))

    group_barrier(z, q)
    for k in range(GRID):
        sq[k] = jnp.zeros((rows, cols), jnp.float32)

    def gather(t, carry):
        @pl.when(t < NB)
        def _():
            own_lines(t, start, True)

        @pl.when(t >= LAG)
        def _():
            b = order_of(z, t - LAG)
            i, j = pick(b, row_of), pick(b, col_of)
            late_line(b, start, True)
            arrived(b, mate)
            arrived(b, mate_other)

            @pl.when(i == z)
            def _():
                xall[b, q] = strip[j]

            block = xall.at[b]
            whole = block[...].reshape(GRID * rows, cols)
            sq[j] += jnp.dot(strip[i], whole, precision=HIGHEST, preferred_element_type=jnp.float32)

            @pl.when(i != j)
            def _():
                sq[i] += lax.dot_general(
                    strip[j], whole, (((1,), (1,)), ((), ())), precision=HIGHEST, preferred_element_type=jnp.float32
                )

        return carry

    lax.fori_loop(0, NB + LAG, gather, 0)

    def sums(j, carry):
        t1, t2, t3 = carry
        x = strip[j]
        on_diag = (local_row + q * rows == local_col) & (z == j)
        return (
            t1 + jnp.sum(jnp.where(on_diag, x, 0.0)),
            t2 + jnp.sum(x * x),
            t3 + jnp.sum(sq[j] * x),
        )

    zero = jnp.float32(0.0)
    t1, t2, t3 = lax.fori_loop(0, GRID, sums, (zero, zero, zero))
    red[me] = as_tile(t1, t2, t3)
    for k in range(GRID):
        res[k] = jnp.zeros((rows, cols), jnp.float32)
    reduce_start(me, red, red_send, red_recv)

    def cube(jj, total_energy):
        j = (q + 1 + jj) % GRID

        def inner(i, carry):
            b, stored = block_of(i, j)

            @pl.when(stored == 1)
            def _():
                whole = xall[b].reshape(GRID * rows, cols)
                res[j] += jnp.dot(sq[i], whole, precision=HIGHEST, preferred_element_type=jnp.float32)

            @pl.when(stored == 0)
            def _():
                whole = xall[b].reshape(GRID * rows, cols)
                res[j] += lax.dot_general(
                    sq[i], whole, (((1,), (1,)), ((), ())), precision=HIGHEST, preferred_element_type=jnp.float32
                )

            return carry

        lax.fori_loop(0, GRID, inner, 0)

        @pl.when(jj == 0)
        def _():
            red[0] = reduce_finish(me, red, red_send, red_recv)

        total = red[0]
        s1, s2, s3 = total[0:1, 0:1], total[1:2, 0:1], total[2:3, 0:1]
        mix = (s2 - s3) / (s1 - s2)
        new = ((1.0 - 2.0 * mix) * strip[j] + (1.0 + mix) * sq[j] - res[j]) / (1.0 - mix)
        res[j] = new
        if not last:
            return total_energy
        total_energy += jnp.sum(res[j] * ham_strip[j])

        @pl.when(jj < GRID - 1)
        def _():
            remote(res.at[j], out.at[q], out_send.at[j], out_recv.at[q], z, j).start()

        @pl.when(jj == GRID - 1)
        def _():
            out[q] = res[j]

        return total_energy

    part = lax.fori_loop(0, GRID, cube, zero)

    def drain(t, carry):
        own_lines(t, wait_send, False)
        late_line(order_of(z, t), wait_send, False)
        return carry

    if last:
        red2[me] = as_tile(2.0 * part)
        lax.fori_loop(0, NB, drain, 0)
        reduce_start(me, red2, red2_send, red2_recv)
        for k in (1, 2, 3):
            j = (q + k) % GRID
            remote(res.at[j], out.at[q], out_send.at[j], out_recv.at[q], z, j).wait_send()
            remote(res.at[j], out.at[j], out_send.at[j], out_recv.at[j], z, j).wait_recv()
        energy[...] = reduce_finish(me, red2, red2_send, red2_recv)
    else:
        lax.fori_loop(0, NB, drain, 0)


def vmem_spec():
    return pl.BlockSpec(memory_space=pltpu.VMEM)


def call_params(which):
    return pltpu.CompilerParams(collective_id=which, has_side_effects=True, vmem_limit_bytes=VMEM_BYTES)


def solution(mesh):
    peers = GRID * GRID
    dma = pltpu.SemaphoreType.DMA

    def local_fn(ham_blk, bounds, n_occ):
        size, cols = ham_blk.shape
        rows = size // GRID
        order = float(cols * mesh.shape["col"])
        f32 = jnp.float32
        strip = jax.ShapeDtypeStruct((GRID, rows, cols), f32)
        smem = pl.BlockSpec(memory_space=pltpu.SMEM)
        ham_strip, dens = pl.pallas_call(
            functools.partial(prepare_kernel, order),
            out_shape=(strip, strip),
            in_specs=[vmem_spec(), smem, smem],
            out_specs=(vmem_spec(), vmem_spec()),
            scratch_shapes=[pltpu.VMEM((peers, 8, 128), f32), dma((GRID,)), dma((GRID,)), dma((peers,)), dma((peers,))],
            compiler_params=call_params(0),
            name="prepare",
        )(ham_blk.reshape(GRID, rows, cols), bounds, n_occ)
        for step in range(STEPS):
            last = step == STEPS - 1
            scratch = [pltpu.VMEM((NB, GRID, rows, cols), f32), pltpu.VMEM((GRID, rows, cols), f32)]
            sems = [dma((NB, GRID)), dma((NB, 2, 4)), dma((peers,)), dma((peers,))]
            red = pltpu.VMEM((peers, 8, 128), f32)
            if last:
                scratch += [pltpu.VMEM((GRID, rows, cols), f32), red, red]
                sems += [dma((peers,)), dma((peers,)), dma((GRID,)), dma((GRID,))]
            else:
                scratch += [red]
            result = pl.pallas_call(
                functools.partial(step_kernel, last),
                out_shape=(strip, jax.ShapeDtypeStruct((8, 128), f32)) if last else strip,
                in_specs=[vmem_spec()] * (2 if last else 1),
                out_specs=(vmem_spec(), vmem_spec()) if last else vmem_spec(),
                scratch_shapes=scratch + sems,
                compiler_params=call_params(1 + step),
                name="purify_last" if last else "purify",
            )(*((dens, ham_strip) if last else (dens,)))
            dens = result[0] if last else result
        return dens.reshape(size, cols), result[1][0, :1]

    spec_mat = P(("spin", "row"), "col")
    return jax.shard_map(
        local_fn, mesh=mesh, in_specs=(spec_mat, P("spin"), P("spin")), out_specs=(spec_mat, P("spin")), check_vma=False
    )
```

```python
import functools

import jax
import jax.numpy as jnp
from jax import lax
from jax.experimental import pallas as pl
from jax.experimental.pallas import tpu as pltpu
from jax.sharding import PartitionSpec as P

STEPS = 3
GRID = 4
PEERS = GRID * GRID
HIGHEST = lax.Precision.HIGHEST
MESH = pl.DeviceIdType.MESH
VMEM_BYTES = 67043328
BLOCKS = ((0, 0), (0, 1), (0, 2), (1, 1), (1, 2), (2, 2), (2, 3), (3, 3), (3, 0), (3, 1))
NB = len(BLOCKS)
ROW_OF = tuple(i for i, _ in BLOCKS)
COL_OF = tuple(j for _, j in BLOCKS)
HALVES = 2
UNITS = HALVES * NB
UNIT_ROW = tuple(ROW_OF[u // HALVES] for u in range(UNITS))
UNIT_COL = tuple(COL_OF[u // HALVES] for u in range(UNITS))
EARLY = (5, 10, 19)
ORDER = (
    (3, 8, 13, 2, 5, 0, 17, 12, 16, 9, 4, 7, 1, 6, 19, 18, 10, 11, 14, 15),
    (0, 13, 2, 9, 16, 17, 4, 12, 10, 3, 5, 19, 6, 18, 11, 8, 14, 1, 15, 7),
    (13, 6, 16, 11, 17, 10, 8, 0, 19, 9, 12, 3, 2, 18, 7, 5, 14, 4, 15, 1),
    (14, 6, 16, 19, 13, 17, 12, 15, 8, 18, 9, 3, 2, 7, 10, 0, 11, 5, 4, 1),
)
WHOLE = tuple(tuple(int(any(row[k] // HALVES == u // HALVES for k in range(t))) for t, u in enumerate(row)) for row in ORDER)
PLACE = (
    (0, 1, 2, 3, 4, 5, 6, 7, 8, 9),
    (2, 4, 6, 0, 1, 3, 5, 7, 8, 9),
    (7, 8, 9, 3, 5, 0, 1, 2, 4, 6),
    (7, 8, 9, 5, 6, 3, 4, 0, 1, 2),
)
FIRST = (0, 3, 5, 7)
COUNT = (3, 2, 2, 3)
COLUMNS = ((0, 1, 2, 3), (1, 2, 0, 3), (2, 3, 0, 1), (3, 0, 1, 2))
SLOTS = 16
LAND, SPARE = (2 * NB + NB) % SLOTS, (2 * NB + NB + 1) % SLOTS
LAG = 5
PARTS = ((0, 512), (512, 896))


def pick(index, values):
    out = jnp.int32(values[-1])
    for k in range(len(values) - 2, -1, -1):
        out = jnp.where(index == k, jnp.int32(values[k]), out)
    return out


def pick2(row, col, table):
    return pick(row * len(table[0]) + col, [v for line in table for v in line])


def slot_of(step, z, b):
    return (NB * step + pick2(z, b, PLACE)) % SLOTS


def block_of(i, j):
    table = [0] * PEERS
    for b, (bi, bj) in enumerate(BLOCKS):
        table[bi * GRID + bj] = b
        table[bj * GRID + bi] = b
    stored = [1 if (k // GRID, k % GRID) in BLOCKS else 0 for k in range(PEERS)]
    at = i * GRID + j
    return pick(at, table), pick(at, stored)


def remote(src, dst, send_sem, recv_sem, z, q):
    return pltpu.make_async_remote_copy(
        src_ref=src, dst_ref=dst, send_sem=send_sem, recv_sem=recv_sem, device_id={"row": z, "col": q}, device_id_type=MESH
    )


def group_barrier(me):
    barrier = pltpu.get_barrier_semaphore()

    def signal(k, carry):
        to = (me + k) % PEERS
        pl.semaphore_signal(barrier, inc=1, device_id={"row": to // GRID, "col": to % GRID}, device_id_type=MESH)
        return carry

    lax.fori_loop(1, PEERS, signal, 0)
    pl.semaphore_wait(barrier, PEERS - 1)


def reduce_copy(k, me, red, send_sems, recv_sems):
    to = (me + k) % PEERS
    return remote(red.at[me], red.at[me], send_sems.at[k], recv_sems.at[me], to // GRID, to % GRID)


def reduce_start(me, red, send_sems, recv_sems):
    def body(k, carry):
        reduce_copy(k, me, red, send_sems, recv_sems).start()
        return carry

    lax.fori_loop(1, PEERS, body, 0)


def reduce_finish(me, red, send_sems, recv_sems):
    def body(k, carry):
        frm = (me + k) % PEERS
        remote(red.at[frm], red.at[frm], send_sems.at[k], recv_sems.at[frm], frm // GRID, frm % GRID).wait_recv()
        reduce_copy(k, me, red, send_sems, recv_sems).wait_send()
        return carry

    lax.fori_loop(1, PEERS, body, 0)
    return jnp.sum(red[...], axis=0)


def as_tile(*sums):
    row = lax.broadcasted_iota(jnp.int32, (8, 128), 0)
    tile = jnp.zeros((8, 128), jnp.float32)
    for k, value in enumerate(sums):
        tile = jnp.where(row == k, value, tile)
    return tile


def purify_kernel(
    order, ham, bounds, n_occ, out, energy, xall, strip, sq, acc, red, red2, total,
    recv, sent, red_send, red_recv, red2_send, red2_recv, ex_send, ex_recv, out_send, out_recv, local_sem, credit,
):
    z, q = lax.axis_index("row"), lax.axis_index("col")
    me = z * GRID + q
    other = (q + 2) % GRID
    mate = q + 1 - 2 * (q % 2)
    mate_other = (mate + 2) % GRID
    rows, cols = strip.shape[1:]
    local_row = lax.broadcasted_iota(jnp.int32, (rows, cols), 0)
    local_col = lax.broadcasted_iota(jnp.int32, (rows, cols), 1)

    def on_diag(j):
        return (local_row + q * rows == local_col) & (z == j)

    half = rows // HALVES

    def part_of(s):
        return pl.ds(pl.multiple_of(s * rows, 8), rows)

    def piece_of(slot, s):
        return xall.at[slot, part_of(s)]

    def unit_at(step, z_at, u, s):
        at = pl.ds(pl.multiple_of(s * rows + (u % HALVES) * half, 8), half)
        return xall.at[slot_of(step, z_at, u // HALVES), at]

    def add_product(out, lhs, slot):
        for lo, hi in PARTS:
            out[:, lo:hi] += jnp.dot(lhs[...], xall[slot, :, lo:hi], precision=HIGHEST, preferred_element_type=jnp.float32)

    def add_mirrored(out, lhs, slot):
        for lo, hi in PARTS:
            out[:, lo:hi] += lax.dot_general(
                lhs[...], xall[slot, lo:hi, :], (((1,), (1,)), ((), ())), precision=HIGHEST, preferred_element_type=jnp.float32
            )

    def is_early(u):
        return functools.reduce(jnp.logical_or, [u == e for e in EARLY])

    def hop(step, src, u, s, line, kind, z_to, q_to):
        return remote(src, unit_at(step, z_to, u, s), sent.at[u, line, kind], recv.at[u, s], z_to, q_to)

    def along(step, src, u, s, line, act):
        origin = pick(u, UNIT_ROW)

        @pl.when((z >= origin) & (z < GRID - 1))
        def _():
            act(hop(step, src, u, s, line, 0, z + 1, q))

        @pl.when((z <= origin) & (z > 0))
        def _():
            act(hop(step, src, u, s, line, 1, z - 1, q))

    def across(step, src, u, s, act):
        act(hop(step, src, u, s, 0, 2, z, other))

    def to_mate(step, src, u, s, line, act):
        act(hop(step, src, u, s, line, 3, z, mate))

    def arrived(step, u, s):
        unit = unit_at(step, z, u, s)
        remote(unit, unit, sent.at[u, 0, 0], recv.at[u, s], z, mate).wait_recv()

    def start(copy):
        copy.start()

    def wait_send(copy):
        copy.wait_send()

    def own_unit(step, n, act):
        u = HALVES * pick(z, FIRST) + n
        src = strip.at[pick(u, UNIT_COL), pl.ds(pl.multiple_of((u % HALVES) * half, 8), half)]
        along(step, src, u, q, 0, act)
        across(step, src, u, q, act)
        to_mate(step, src, u, q, 0, act)

    def publish(step, jj):
        b = pick(z, FIRST) + jj
        xall[slot_of(step, z, b), part_of(q)] = strip[pick(b, COL_OF)]
        for h in range(HALVES):
            own_unit(step, HALVES * jj + h, start)

    def relay(step, t, act, waits):
        u = pick2(z, t, ORDER)
        early = is_early(u)

        @pl.when(pick(u, UNIT_ROW) != z)
        def _():
            if waits:
                arrived(step, u, q)
            src = unit_at(step, z, u, q)
            along(step, src, u, q, 0, act)

            @pl.when(jnp.logical_not(early))
            def _():
                across(step, src, u, q, act)

            to_mate(step, src, u, q, 0, act)

        @pl.when(early)
        def _():
            if waits:
                arrived(step, u, other)
            src = unit_at(step, z, u, other)
            along(step, src, u, other, 1, act)
            to_mate(step, src, u, other, 1, act)

    def late(step, u, act, waits):
        @pl.when(jnp.logical_not(is_early(u)))
        def _():
            if waits:
                arrived(step, u, other)
            to_mate(step, unit_at(step, z, u, other), u, other, 1, act)

    group_barrier(me)

    def exchange(k):
        to = (q + k) % GRID
        return remote(ham.at[part_of(to)], strip.at[q], ex_send.at[k], ex_recv.at[q], z, to)

    for k in (2, 3, 1):
        exchange(k).start()
    load = pltpu.make_async_copy(ham, xall.at[SPARE], local_sem)
    load.start()
    load.wait()
    part = jnp.float32(0.0)
    for s in range(GRID):
        part += jnp.sum(jnp.where((local_row + s * rows == local_col) & (z == q), xall[SPARE, s * rows : (s + 1) * rows], 0.0))
    red[me] = as_tile(part)
    strip[q] = xall[SPARE, part_of(q)]
    reduce_start(me, red, red_send, red_recv)
    mu = reduce_finish(me, red, red_send, red_recv)[0:1, 0:1] / order
    occ = jnp.full((1, 1), n_occ[0].astype(jnp.float32))
    low, high = jnp.full((1, 1), bounds[0]), jnp.full((1, 1), bounds[1])
    lam = jnp.minimum(occ / (high - mu), (order - occ) / (mu - low))
    scale, shift = lam / order, occ / order

    def initial(jj, carry):
        j = pick2(z, jj, COLUMNS)

        @pl.when(j != q)
        def _():
            remote(ham.at[part_of(0)], strip.at[j], ex_send.at[0], ex_recv.at[j], z, j).wait_recv()

        strip[j] = scale * (jnp.where(on_diag(j), mu, 0.0) - strip[j]) + jnp.where(on_diag(j), shift, 0.0)

        @pl.when(jj < pick(z, COUNT))
        def _():
            publish(0, jj)

        return carry

    lax.fori_loop(0, GRID, initial, 0)
    for k in (1, 2, 3):
        exchange(k).wait_send()

    def one_step(step, carry):
        last = step == STEPS - 1
        for k in range(GRID):
            sq[k] = jnp.zeros((rows, cols), jnp.float32)

        def gather(t, carry):
            @pl.when(t < UNITS)
            def _():
                relay(step, t, start, True)

            @pl.when(t >= LAG)
            def _():
                u = pick2(z, t - LAG, ORDER)
                i, j = pick(u, UNIT_ROW), pick(u, UNIT_COL)
                late(step, u, start, True)
                arrived(step, u, mate)
                arrived(step, u, mate_other)
                whole = pick2(z, t - LAG, WHOLE) == 1
                slot = slot_of(step, z, u // HALVES)

                @pl.when(whole)
                def _():
                    add_product(sq.at[j], strip.at[i], slot)

                @pl.when(whole & (i != j))
                def _():
                    add_mirrored(sq.at[i], strip.at[j], slot)

            return carry

        lax.fori_loop(0, UNITS + LAG, gather, 0)

        def sums(j, carry):
            t1, t2, t3 = carry
            x = strip[j]
            return (
                t1 + jnp.sum(jnp.where(on_diag(j), x, 0.0)),
                t2 + jnp.sum(x * x),
                t3 + jnp.sum(sq[j] * x),
            )

        zero = jnp.float32(0.0)
        red[me] = as_tile(*lax.fori_loop(0, GRID, sums, (zero, zero, zero)))
        acc[...] = jnp.zeros((rows, cols), jnp.float32)
        reduce_start(me, red, red_send, red_recv)

        def cube(jj, carry):
            j = jnp.where(last, (q + 1 + jj) % GRID, pick2(z, jj, COLUMNS))

            def inner(i, carry):
                b, stored = block_of(i, j)
                slot = slot_of(step, z, b)

                @pl.when(stored == 1)
                def _():
                    add_product(acc, sq.at[i], slot)

                @pl.when(stored == 0)
                def _():
                    add_mirrored(acc, sq.at[i], slot)

                return carry

            lax.fori_loop(0, GRID, inner, 0)

            @pl.when(jj == 0)
            def _():
                def drain(t, carry):
                    @pl.when(t < HALVES * pick(z, COUNT))
                    def _():
                        own_unit(step, t, wait_send)

                    relay(step, t, wait_send, False)
                    late(step, pick2(z, t, ORDER), wait_send, False)
                    return carry

                lax.fori_loop(0, UNITS, drain, 0)
                total[...] = reduce_finish(me, red, red_send, red_recv)

            sums_v = total[...]
            s1, s2, s3 = sums_v[0:1, 0:1], sums_v[1:2, 0:1], sums_v[2:3, 0:1]
            mix = (s2 - s3) / (s1 - s2)
            strip[j] = ((1.0 - 2.0 * mix) * strip[j] + (1.0 + mix) * sq[j] - acc[...]) / (1.0 - mix)
            acc[...] = jnp.zeros((rows, cols), jnp.float32)

            @pl.when(jnp.logical_not(last) & (jj < 2))
            def _():
                publish(step + 1, jj)

            @pl.when(last & (jj < GRID - 1))
            def _():
                remote(strip.at[j], piece_of(LAND, q), out_send.at[j], out_recv.at[q], z, j).start()

            @pl.when(last & (jj == GRID - 1))
            def _():
                xall[LAND, part_of(q)] = strip[j]

            return carry

        @pl.when(last)
        def _():
            pltpu.make_async_copy(ham, xall.at[SPARE], local_sem).start()

        lax.fori_loop(0, GRID, cube, 0)

        @pl.when(jnp.logical_not(last))
        def _():
            @pl.when(z < GRID - 1)
            def _():
                pl.semaphore_signal(credit, inc=1, device_id={"row": z + 1, "col": q}, device_id_type=MESH)

            @pl.when(z > 0)
            def _():
                pl.semaphore_signal(credit, inc=1, device_id={"row": z - 1, "col": q}, device_id_type=MESH)

            pl.semaphore_signal(credit, inc=1, device_id={"row": z, "col": other}, device_id_type=MESH)
            pl.semaphore_signal(credit, inc=1, device_id={"row": z, "col": mate}, device_id_type=MESH)
            pl.semaphore_wait(credit, pick(z, (3, 4, 4, 3)))

            @pl.when(pick(z, COUNT) == 3)
            def _():
                publish(step + 1, 2)

        return carry

    lax.fori_loop(0, STEPS, one_step, 0)

    pltpu.make_async_copy(ham, xall.at[SPARE], local_sem).wait()
    for k in (1, 2, 3):
        j = (q + k) % GRID
        remote(strip.at[j], piece_of(LAND, q), out_send.at[j], out_recv.at[q], z, j).wait_send()
        remote(strip.at[j], piece_of(LAND, j), out_send.at[j], out_recv.at[j], z, j).wait_recv()
    store = pltpu.make_async_copy(xall.at[LAND], out, local_sem)
    store.start()
    part = jnp.float32(0.0)
    for s in range(GRID):
        part += jnp.sum(xall[LAND, s * rows : (s + 1) * rows] * xall[SPARE, s * rows : (s + 1) * rows])
    red2[me] = as_tile(2.0 * part)
    store.wait()
    reduce_start(me, red2, red2_send, red2_recv)
    energy[...] = reduce_finish(me, red2, red2_send, red2_recv)


def solution(mesh):
    def local_fn(ham_blk, bounds, n_occ):
        size, cols = ham_blk.shape
        rows = size // GRID
        order = float(cols * mesh.shape["col"])
        f32 = jnp.float32
        dma = pltpu.SemaphoreType.DMA
        strip = (GRID, rows, cols)
        smem = pl.BlockSpec(memory_space=pltpu.SMEM)
        anywhere = pl.BlockSpec(memory_space=pl.ANY)
        red = pltpu.VMEM((PEERS, 8, 128), f32)
        density, energy = pl.pallas_call(
            functools.partial(purify_kernel, order),
            out_shape=(jax.ShapeDtypeStruct((size, cols), f32), jax.ShapeDtypeStruct((8, 128), f32)),
            in_specs=[anywhere, smem, smem],
            out_specs=(anywhere, pl.BlockSpec(memory_space=pltpu.VMEM)),
            scratch_shapes=[
                pltpu.VMEM((SLOTS, size, cols), f32),
                pltpu.VMEM(strip, f32),
                pltpu.VMEM(strip, f32),
                pltpu.VMEM((rows, cols), f32),
                red,
                red,
                pltpu.VMEM((8, 128), f32),
                dma((UNITS, GRID)),
                dma((UNITS, 2, 4)),
                dma((PEERS,)),
                dma((PEERS,)),
                dma((PEERS,)),
                dma((PEERS,)),
                dma((GRID,)),
                dma((GRID,)),
                dma((GRID,)),
                dma((GRID,)),
                dma,
                pltpu.SemaphoreType.REGULAR,
            ],
            compiler_params=pltpu.CompilerParams(collective_id=0, has_side_effects=True, vmem_limit_bytes=VMEM_BYTES),
            name="purify",
        )(ham_blk, bounds, n_occ)
        return density, energy[0, :1]

    spec_mat = P(("spin", "row"), "col")
    return jax.shard_map(
        local_fn, mesh=mesh, in_specs=(spec_mat, P("spin"), P("spin")), out_specs=(spec_mat, P("spin")), check_vma=False
    )
```

```python
import functools

import jax
import jax.numpy as jnp
from jax import lax
from jax.experimental import pallas as pl
from jax.experimental.pallas import tpu as pltpu
from jax.sharding import PartitionSpec as P

STEPS = 3
GRID = 4
PEERS = GRID * GRID
HIGHEST = lax.Precision.HIGHEST
MESH = pl.DeviceIdType.MESH
VMEM_BYTES = 67043328
BLOCKS = ((0, 0), (0, 1), (0, 2), (1, 1), (1, 2), (2, 2), (2, 3), (3, 3), (3, 0), (3, 1))
NB = len(BLOCKS)
ROW_OF = tuple(i for i, _ in BLOCKS)
COL_OF = tuple(j for _, j in BLOCKS)
HALVES = 2
UNITS = HALVES * NB
UNIT_ROW = tuple(ROW_OF[u // HALVES] for u in range(UNITS))
UNIT_COL = tuple(COL_OF[u // HALVES] for u in range(UNITS))
EARLY = (5, 10, 19)
ORDER = (
    (3, 8, 13, 2, 5, 0, 17, 12, 16, 9, 4, 7, 1, 6, 19, 18, 10, 11, 14, 15),
    (0, 13, 2, 9, 16, 17, 4, 12, 10, 3, 5, 19, 6, 18, 11, 8, 14, 1, 15, 7),
    (13, 6, 16, 11, 17, 10, 8, 0, 19, 9, 12, 3, 2, 18, 7, 5, 14, 4, 15, 1),
    (14, 6, 16, 19, 13, 17, 12, 15, 8, 18, 9, 3, 2, 7, 10, 0, 11, 5, 4, 1),
)
WHOLE = tuple(tuple(int(any(row[k] // HALVES == u // HALVES for k in range(t))) for t, u in enumerate(row)) for row in ORDER)
PLACE = (
    (0, 1, 2, 3, 4, 5, 6, 7, 8, 9),
    (2, 4, 6, 0, 1, 3, 5, 7, 8, 9),
    (7, 8, 9, 3, 5, 0, 1, 2, 4, 6),
    (7, 8, 9, 5, 6, 3, 4, 0, 1, 2),
)
FIRST = (0, 3, 5, 7)
COUNT = (3, 2, 2, 3)
COLUMNS = ((0, 1, 2, 3), (1, 2, 0, 3), (2, 3, 0, 1), (3, 0, 1, 2))
SLOTS = 16
LAND, SPARE = (2 * NB + NB) % SLOTS, (2 * NB + NB + 1) % SLOTS
LAG, DOT_LAG = 5, 6
PARTS = ((0, 512), (512, 896))


def pick(index, values):
    out = jnp.int32(values[-1])
    for k in range(len(values) - 2, -1, -1):
        out = jnp.where(index == k, jnp.int32(values[k]), out)
    return out


def pick2(row, col, table):
    return pick(row * len(table[0]) + col, [v for line in table for v in line])


def slot_of(step, z, b):
    return (NB * step + pick2(z, b, PLACE)) % SLOTS


def block_of(i, j):
    table = [0] * PEERS
    for b, (bi, bj) in enumerate(BLOCKS):
        table[bi * GRID + bj] = b
        table[bj * GRID + bi] = b
    stored = [1 if (k // GRID, k % GRID) in BLOCKS else 0 for k in range(PEERS)]
    at = i * GRID + j
    return pick(at, table), pick(at, stored)


def remote(src, dst, send_sem, recv_sem, z, q):
    return pltpu.make_async_remote_copy(
        src_ref=src, dst_ref=dst, send_sem=send_sem, recv_sem=recv_sem, device_id={"row": z, "col": q}, device_id_type=MESH
    )


def group_barrier(me):
    barrier = pltpu.get_barrier_semaphore()

    def signal(k, carry):
        to = (me + k) % PEERS
        pl.semaphore_signal(barrier, inc=1, device_id={"row": to // GRID, "col": to % GRID}, device_id_type=MESH)
        return carry

    lax.fori_loop(1, PEERS, signal, 0)
    pl.semaphore_wait(barrier, PEERS - 1)


def reduce_copy(k, me, red, send_sems, recv_sems):
    to = (me + k) % PEERS
    return remote(red.at[me], red.at[me], send_sems.at[k], recv_sems.at[me], to // GRID, to % GRID)


def reduce_start(me, red, send_sems, recv_sems):
    def body(k, carry):
        reduce_copy(k, me, red, send_sems, recv_sems).start()
        return carry

    lax.fori_loop(1, PEERS, body, 0)


def reduce_finish(me, red, send_sems, recv_sems):
    def body(k, carry):
        frm = (me + k) % PEERS
        remote(red.at[frm], red.at[frm], send_sems.at[k], recv_sems.at[frm], frm // GRID, frm % GRID).wait_recv()
        reduce_copy(k, me, red, send_sems, recv_sems).wait_send()
        return carry

    lax.fori_loop(1, PEERS, body, 0)
    return jnp.sum(red[...], axis=0)


def as_tile(*sums):
    row = lax.broadcasted_iota(jnp.int32, (8, 128), 0)
    tile = jnp.zeros((8, 128), jnp.float32)
    for k, value in enumerate(sums):
        tile = jnp.where(row == k, value, tile)
    return tile


def purify_kernel(
    order, ham, bounds, n_occ, out, energy, xall, strip, sq, acc, red, red2, total,
    recv, sent, red_send, red_recv, red2_send, red2_recv, ex_send, ex_recv, out_send, out_recv, local_sem, credit,
):
    z, q = lax.axis_index("row"), lax.axis_index("col")
    me = z * GRID + q
    other = (q + 2) % GRID
    mate = q + 1 - 2 * (q % 2)
    mate_other = (mate + 2) % GRID
    rows, cols = strip.shape[1:]
    local_row = lax.broadcasted_iota(jnp.int32, (rows, cols), 0)
    local_col = lax.broadcasted_iota(jnp.int32, (rows, cols), 1)

    def on_diag(j):
        return (local_row + q * rows == local_col) & (z == j)

    half = rows // HALVES

    def part_of(s):
        return pl.ds(pl.multiple_of(s * rows, 8), rows)

    def piece_of(slot, s):
        return xall.at[slot, part_of(s)]

    def unit_at(step, z_at, u, s):
        at = pl.ds(pl.multiple_of(s * rows + (u % HALVES) * half, 8), half)
        return xall.at[slot_of(step, z_at, u // HALVES), at]

    def add_product(out, lhs, slot):
        for lo, hi in PARTS:
            out[:, lo:hi] += jnp.dot(lhs[...], xall[slot, :, lo:hi], precision=HIGHEST, preferred_element_type=jnp.float32)

    def add_mirrored(out, lhs, slot):
        for lo, hi in PARTS:
            out[:, lo:hi] += lax.dot_general(
                lhs[...], xall[slot, lo:hi, :], (((1,), (1,)), ((), ())), precision=HIGHEST, preferred_element_type=jnp.float32
            )

    def is_early(u):
        return functools.reduce(jnp.logical_or, [u == e for e in EARLY])

    def hop(step, src, u, s, line, kind, z_to, q_to):
        return remote(src, unit_at(step, z_to, u, s), sent.at[u, line, kind], recv.at[u, s], z_to, q_to)

    def along(step, src, u, s, line, act):
        origin = pick(u, UNIT_ROW)

        @pl.when((z >= origin) & (z < GRID - 1))
        def _():
            act(hop(step, src, u, s, line, 0, z + 1, q))

        @pl.when((z <= origin) & (z > 0))
        def _():
            act(hop(step, src, u, s, line, 1, z - 1, q))

    def across(step, src, u, s, act):
        act(hop(step, src, u, s, 0, 2, z, other))

    def to_mate(step, src, u, s, line, act):
        act(hop(step, src, u, s, line, 3, z, mate))

    def arrived(step, u, s):
        unit = unit_at(step, z, u, s)
        remote(unit, unit, sent.at[u, 0, 0], recv.at[u, s], z, mate).wait_recv()

    def start(copy):
        copy.start()

    def wait_send(copy):
        copy.wait_send()

    def own_unit(step, n, act):
        u = HALVES * pick(z, FIRST) + n
        src = strip.at[pick(u, UNIT_COL), pl.ds(pl.multiple_of((u % HALVES) * half, 8), half)]
        along(step, src, u, q, 0, act)
        across(step, src, u, q, act)
        to_mate(step, src, u, q, 0, act)

    def publish(step, jj):
        b = pick(z, FIRST) + jj
        xall[slot_of(step, z, b), part_of(q)] = strip[pick(b, COL_OF)]
        for h in range(HALVES):
            own_unit(step, HALVES * jj + h, start)

    def relay(step, t, act, waits):
        u = pick2(z, t, ORDER)
        early = is_early(u)

        @pl.when(pick(u, UNIT_ROW) != z)
        def _():
            if waits:
                arrived(step, u, q)
            src = unit_at(step, z, u, q)
            along(step, src, u, q, 0, act)

            @pl.when(jnp.logical_not(early))
            def _():
                across(step, src, u, q, act)

            to_mate(step, src, u, q, 0, act)

        @pl.when(early)
        def _():
            if waits:
                arrived(step, u, other)
            src = unit_at(step, z, u, other)
            along(step, src, u, other, 1, act)
            to_mate(step, src, u, other, 1, act)

    def late(step, u, act, waits):
        @pl.when(jnp.logical_not(is_early(u)))
        def _():
            if waits:
                arrived(step, u, other)
            to_mate(step, unit_at(step, z, u, other), u, other, 1, act)

    group_barrier(me)

    def exchange(k):
        to = (q + k) % GRID
        return remote(ham.at[part_of(to)], strip.at[q], ex_send.at[k], ex_recv.at[q], z, to)

    for k in (2, 3, 1):
        exchange(k).start()
    load = pltpu.make_async_copy(ham, xall.at[SPARE], local_sem)
    load.start()
    load.wait()
    part = jnp.float32(0.0)
    for s in range(GRID):
        part += jnp.sum(jnp.where((local_row + s * rows == local_col) & (z == q), xall[SPARE, s * rows : (s + 1) * rows], 0.0))
    red[me] = as_tile(part)
    strip[q] = xall[SPARE, part_of(q)]
    reduce_start(me, red, red_send, red_recv)
    mu = reduce_finish(me, red, red_send, red_recv)[0:1, 0:1] / order
    occ = jnp.full((1, 1), n_occ[0].astype(jnp.float32))
    low, high = jnp.full((1, 1), bounds[0]), jnp.full((1, 1), bounds[1])
    lam = jnp.minimum(occ / (high - mu), (order - occ) / (mu - low))
    scale, shift = lam / order, occ / order

    def initial(jj, carry):
        j = pick2(z, jj, COLUMNS)

        @pl.when(j != q)
        def _():
            remote(ham.at[part_of(0)], strip.at[j], ex_send.at[0], ex_recv.at[j], z, j).wait_recv()

        strip[j] = scale * (jnp.where(on_diag(j), mu, 0.0) - strip[j]) + jnp.where(on_diag(j), shift, 0.0)

        @pl.when(jj < pick(z, COUNT))
        def _():
            publish(0, jj)

        return carry

    lax.fori_loop(0, GRID, initial, 0)
    for k in (1, 2, 3):
        exchange(k).wait_send()

    def one_step(step, carry):
        last = step == STEPS - 1
        for k in range(GRID):
            sq[k] = jnp.zeros((rows, cols), jnp.float32)

        def gather(t, carry):
            @pl.when(t < UNITS)
            def _():
                relay(step, t, start, True)

            @pl.when((t >= LAG) & (t < UNITS + LAG))
            def _():
                late(step, pick2(z, t - LAG, ORDER), start, True)

            @pl.when(t >= DOT_LAG)
            def _():
                u = pick2(z, t - DOT_LAG, ORDER)
                i, j = pick(u, UNIT_ROW), pick(u, UNIT_COL)
                arrived(step, u, mate)
                arrived(step, u, mate_other)
                whole = pick2(z, t - DOT_LAG, WHOLE) == 1
                slot = slot_of(step, z, u // HALVES)

                @pl.when(whole)
                def _():
                    add_product(sq.at[j], strip.at[i], slot)

                @pl.when(whole & (i != j))
                def _():
                    add_mirrored(sq.at[i], strip.at[j], slot)

            return carry

        lax.fori_loop(0, UNITS + DOT_LAG, gather, 0)

        def sums(j, carry):
            t1, t2, t3 = carry
            x = strip[j]
            return (
                t1 + jnp.sum(jnp.where(on_diag(j), x, 0.0)),
                t2 + jnp.sum(x * x),
                t3 + jnp.sum(sq[j] * x),
            )

        zero = jnp.float32(0.0)
        red[me] = as_tile(*lax.fori_loop(0, GRID, sums, (zero, zero, zero)))
        acc[...] = jnp.zeros((rows, cols), jnp.float32)
        reduce_start(me, red, red_send, red_recv)

        def cube(jj, carry):
            j = jnp.where(last, (q + 1 + jj) % GRID, pick2(z, jj, COLUMNS))

            def inner(i, carry):
                b, stored = block_of(i, j)
                slot = slot_of(step, z, b)

                @pl.when(stored == 1)
                def _():
                    add_product(acc, sq.at[i], slot)

                @pl.when(stored == 0)
                def _():
                    add_mirrored(acc, sq.at[i], slot)

                return carry

            lax.fori_loop(0, GRID, inner, 0)

            @pl.when(jj == 0)
            def _():
                def drain(t, carry):
                    @pl.when(t < HALVES * pick(z, COUNT))
                    def _():
                        own_unit(step, t, wait_send)

                    relay(step, t, wait_send, False)
                    late(step, pick2(z, t, ORDER), wait_send, False)
                    return carry

                lax.fori_loop(0, UNITS, drain, 0)
                total[...] = reduce_finish(me, red, red_send, red_recv)

            sums_v = total[...]
            s1, s2, s3 = sums_v[0:1, 0:1], sums_v[1:2, 0:1], sums_v[2:3, 0:1]
            mix = (s2 - s3) / (s1 - s2)
            strip[j] = ((1.0 - 2.0 * mix) * strip[j] + (1.0 + mix) * sq[j] - acc[...]) / (1.0 - mix)
            acc[...] = jnp.zeros((rows, cols), jnp.float32)

            @pl.when(jnp.logical_not(last) & (jj < 2))
            def _():
                publish(step + 1, jj)

            @pl.when(last & (jj < GRID - 1))
            def _():
                remote(strip.at[j], piece_of(LAND, q), out_send.at[j], out_recv.at[q], z, j).start()

            @pl.when(last & (jj == GRID - 1))
            def _():
                xall[LAND, part_of(q)] = strip[j]

            return carry

        @pl.when(last)
        def _():
            pltpu.make_async_copy(ham, xall.at[SPARE], local_sem).start()

        lax.fori_loop(0, GRID, cube, 0)

        @pl.when(jnp.logical_not(last))
        def _():
            @pl.when(z < GRID - 1)
            def _():
                pl.semaphore_signal(credit, inc=1, device_id={"row": z + 1, "col": q}, device_id_type=MESH)

            @pl.when(z > 0)
            def _():
                pl.semaphore_signal(credit, inc=1, device_id={"row": z - 1, "col": q}, device_id_type=MESH)

            pl.semaphore_signal(credit, inc=1, device_id={"row": z, "col": other}, device_id_type=MESH)
            pl.semaphore_signal(credit, inc=1, device_id={"row": z, "col": mate}, device_id_type=MESH)
            pl.semaphore_wait(credit, pick(z, (3, 4, 4, 3)))

            @pl.when(pick(z, COUNT) == 3)
            def _():
                publish(step + 1, 2)

        return carry

    lax.fori_loop(0, STEPS, one_step, 0)

    pltpu.make_async_copy(ham, xall.at[SPARE], local_sem).wait()
    for k in (1, 2, 3):
        j = (q + k) % GRID
        remote(strip.at[j], piece_of(LAND, q), out_send.at[j], out_recv.at[q], z, j).wait_send()
        remote(strip.at[j], piece_of(LAND, j), out_send.at[j], out_recv.at[j], z, j).wait_recv()
    store = pltpu.make_async_copy(xall.at[LAND], out, local_sem)
    store.start()
    part = jnp.float32(0.0)
    for s in range(GRID):
        part += jnp.sum(xall[LAND, s * rows : (s + 1) * rows] * xall[SPARE, s * rows : (s + 1) * rows])
    red2[me] = as_tile(2.0 * part)
    store.wait()
    reduce_start(me, red2, red2_send, red2_recv)
    energy[...] = reduce_finish(me, red2, red2_send, red2_recv)


def solution(mesh):
    def local_fn(ham_blk, bounds, n_occ):
        size, cols = ham_blk.shape
        rows = size // GRID
        order = float(cols * mesh.shape["col"])
        f32 = jnp.float32
        dma = pltpu.SemaphoreType.DMA
        strip = (GRID, rows, cols)
        smem = pl.BlockSpec(memory_space=pltpu.SMEM)
        anywhere = pl.BlockSpec(memory_space=pl.ANY)
        red = pltpu.VMEM((PEERS, 8, 128), f32)
        density, energy = pl.pallas_call(
            functools.partial(purify_kernel, order),
            out_shape=(jax.ShapeDtypeStruct((size, cols), f32), jax.ShapeDtypeStruct((8, 128), f32)),
            in_specs=[anywhere, smem, smem],
            out_specs=(anywhere, pl.BlockSpec(memory_space=pltpu.VMEM)),
            scratch_shapes=[
                pltpu.VMEM((SLOTS, size, cols), f32),
                pltpu.VMEM(strip, f32),
                pltpu.VMEM(strip, f32),
                pltpu.VMEM((rows, cols), f32),
                red,
                red,
                pltpu.VMEM((8, 128), f32),
                dma((UNITS, GRID)),
                dma((UNITS, 2, 4)),
                dma((PEERS,)),
                dma((PEERS,)),
                dma((PEERS,)),
                dma((PEERS,)),
                dma((GRID,)),
                dma((GRID,)),
                dma((GRID,)),
                dma((GRID,)),
                dma,
                pltpu.SemaphoreType.REGULAR,
            ],
            compiler_params=pltpu.CompilerParams(collective_id=0, has_side_effects=True, vmem_limit_bytes=VMEM_BYTES),
            name="purify",
        )(ham_blk, bounds, n_occ)
        return density, energy[0, :1]

    spec_mat = P(("spin", "row"), "col")
    return jax.shard_map(
        local_fn, mesh=mesh, in_specs=(spec_mat, P("spin"), P("spin")), out_specs=(spec_mat, P("spin")), check_vma=False
    )
```
